32 devices in a mesh: sib: 4 (over y, x), wide: 8 (over z, core).
Axes of the slice: x: 2, y: 2, z: 4, core: 2. Of those that a mesh axis runs over, the one named last changes fastest.
Arguments:
- right_side: float32 [128, 8, 2048], P(None, 'wide', 'sib'), may hold values from -6 to 6
- tree_order: int32 [8, 2048], P('wide', 'sib'), may hold values from 0 to 2047, each once within a row
- x_start: float32 [128, 8, 2048], P(None, 'wide', 'sib'), may hold values from -6 to 6
- tangent_start: float32 [128, 8, 2048], P(None, 'wide', 'sib'), may hold values from -3 to 3
- dense_kernel: float32 [8, 4, 512, 512], P('wide', 'sib'), may hold values from -0.25 to 0.25
- dense_deriv: float32 [8, 4, 512, 512], P('wide', 'sib'), may hold values from -0.25 to 0.25
- leaf_basis: float32 [8, 4, 512, 256], P('wide', 'sib'), may hold values from -0.25 to 0.25
- transfer: float32 [8, 4, 256, 256], P('wide', 'sib'), may hold values from -0.375 to 0.375
- sibling_kernel: float32 [8, 4, 3, 256, 256], P('wide', 'sib'), may hold values from -0.21875 to 0.21875
- sibling_deriv: float32 [8, 4, 3, 256, 256], P('wide', 'sib'), may hold values from -0.21875 to 0.21875
- partner_list: int32 [8, 4], P('wide'), may hold values from 0 to 7, as said below
- parent_kernel: float32 [8, 4, 256, 256], P('wide'), may hold values from -0.1875 to 0.1875
- parent_deriv: float32 [8, 4, 256, 256], P('wide'), may hold values from -0.1875 to 0.1875
Outputs:
- solution: float32 [128, 8, 2048], P(None, 'wide', 'sib')
- tangent: float32 [128, 8, 2048], P(None, 'wide', 'sib')
The draws below stay inside these ranges and needn't reach their ends.
Inputs may be any that keep to these rules, and one draw needn't show every extreme that they name: `partner_list`: row p names 4 different parent clusters, none of them p. `tree_order`: each row holds every position 0 .. 2047 once.
All inputs are finite; a program needn't handle non-finite values.
Results may differ from the reference program's by a relative error of at most 0.0001.
Values sent between devices are 32-bit elements; how exact they have to be, the bound alone decides.
No kernel may reach another device: no remote copies, remote signals or barrier semaphores. Data moves between devices by JAX's collectives and lax.ppermute only.
A program may use at most 64 MiB of HBM per device.

```python
import jax
import jax.numpy as jnp
from jax import lax

LEAF = 512
RHS = 128
RANK = 256
NB_PAR = 4
ITERS = 2
PARENTS = 8
PTS_PAR = 2048
N_SIB = 4


def draw_partner_list(key, part):
    key = jax.random.fold_in(key, 7)
    scores = jax.random.randint(key, (PARENTS, PARENTS - 1), 0, 1 << 20)
    scores = scores * PARENTS + jnp.arange(PARENTS - 1, dtype=jnp.int32)[None, :]
    chosen = lax.top_k(scores, NB_PAR)[1].astype(jnp.int32)
    rows = jnp.arange(PARENTS, dtype=jnp.int32)[:, None]
    return ((rows + chosen + 1) % PARENTS).astype(jnp.int32)


def block_scale(stream_key, dims, split, low, high):
    def one(dim, parts):
        draws = jax.random.uniform(jax.random.fold_in(jax.random.fold_in(stream_key, 6), dim), (parts,), jnp.float32, low / len(split), high / len(split))
        return jnp.repeat(jnp.exp(draws), dims[dim] // parts).reshape((-1,) + (1,) * (len(dims) - dim - 1))

    loudness = one(*split[0])
    for cut in split[1:]:
        loudness = loudness * one(*cut)
    return loudness


def normal_values(key, extent, scale, most, shards=(), kind=jnp.bfloat16):
    result = jax.random.normal(key, extent, jnp.float32) * scale
    if len(shards) > 0:
        result = block_scale(key, extent, shards, -0.22, 0.18) * result
    return jnp.clip(result, min=-most, max=most).astype(kind)


def setup_inputs(seed: int = 0) -> dict:
    keys = jax.random.split(jax.random.key(seed), 14)
    return {
        "right_side": normal_values(keys[0], (RHS, PARENTS, PTS_PAR), 1.0, 6.0, ((1, 8), (2, 4)), jnp.float32),
        "tree_order": jax.vmap(lambda own: jax.random.permutation(own, PTS_PAR))(jax.random.split(keys[1], PARENTS)).reshape((PARENTS, PTS_PAR)).astype(jnp.int32),
        "x_start": normal_values(keys[2], (RHS, PARENTS, PTS_PAR), 1.0, 6.0, ((1, 8), (2, 4)), jnp.float32),
        "tangent_start": normal_values(keys[3], (RHS, PARENTS, PTS_PAR), 0.5, 3.0, ((1, 8), (2, 4)), jnp.float32),
        "dense_kernel": normal_values(keys[4], (PARENTS, N_SIB, LEAF, LEAF), LEAF ** -0.5, 0.25, ((0, 8), (1, 4)), jnp.float32),
        "dense_deriv": normal_values(keys[5], (PARENTS, N_SIB, LEAF, LEAF), LEAF ** -0.5, 0.25, ((0, 8), (1, 4)), jnp.float32),
        "leaf_basis": normal_values(keys[6], (PARENTS, N_SIB, LEAF, RANK), LEAF ** -0.5, 0.25, ((0, 8), (1, 4)), jnp.float32),
        "transfer": normal_values(keys[7], (PARENTS, N_SIB, RANK, RANK), RANK ** -0.5, 0.375, ((0, 8), (1, 4)), jnp.float32),
        "sibling_kernel": normal_values(keys[8], (PARENTS, N_SIB, N_SIB - 1, RANK, RANK), (RANK * (N_SIB - 1)) ** -0.5, 0.21875, ((0, 8), (1, 4)), jnp.float32),
        "sibling_deriv": normal_values(keys[9], (PARENTS, N_SIB, N_SIB - 1, RANK, RANK), (RANK * (N_SIB - 1)) ** -0.5, 0.21875, ((0, 8), (1, 4)), jnp.float32),
        "partner_list": draw_partner_list(jax.random.fold_in(keys[13], 71), 0),
        "parent_kernel": normal_values(keys[11], (PARENTS, NB_PAR, RANK, RANK), (RANK * NB_PAR) ** -0.5, 0.1875, ((0, 8),), jnp.float32),
        "parent_deriv": normal_values(keys[12], (PARENTS, NB_PAR, RANK, RANK), (RANK * NB_PAR) ** -0.5, 0.1875, ((0, 8),), jnp.float32),
    }


highest = lax.Precision.HIGHEST
relax_step = 0.3
noise_level = 1.0


def contract(form, left, right):
    return jnp.einsum(form, left, right, precision=highest, preferred_element_type=jnp.float32)


def siblings(coeff, couple):
    total = jnp.zeros_like(coeff)
    for offset in range(1, N_SIB):
        total = total + contract('rpsk,pskm->rpsm', jnp.roll(coeff, -offset, axis=2), couple[:, :, offset - 1])
    return total


def reference(right_side, tree_order, x_start, tangent_start, dense_kernel, dense_deriv, leaf_basis, transfer, sibling_kernel, sibling_deriv, partner_list, parent_kernel, parent_deriv):
    shape = (RHS, PARENTS, N_SIB, LEAF)
    order = jnp.broadcast_to(tree_order[None].astype(jnp.int32), right_side.shape)
    rhs = jnp.take_along_axis(right_side, order, axis=2).reshape(shape)
    x = x_start.reshape(shape)
    dx = tangent_start.reshape(shape)
    for step in range(ITERS):
        ax = contract('rpsl,pslk->rpsk', x, leaf_basis)
        adx = contract('rpsl,pslk->rpsk', dx, leaf_basis)
        gx = siblings(ax, sibling_kernel)
        gdx = siblings(ax, sibling_deriv) + siblings(adx, sibling_kernel)
        px = contract('rpsk,pskm->rpm', ax, transfer)
        pdx = contract('rpsk,pskm->rpm', adx, transfer)
        cx = jnp.take(px, partner_list.astype(jnp.int32), axis=1)
        cdx = jnp.take(pdx, partner_list.astype(jnp.int32), axis=1)
        hx = contract('rpbk,pbkm->rpm', cx, parent_kernel)
        hdx = contract('rpbk,pbkm->rpm', cx, parent_deriv) + contract('rpbk,pbkm->rpm', cdx, parent_kernel)
        zx = gx + contract('rpm,pskm->rpsk', hx, transfer)
        zdx = gdx + contract('rpm,pskm->rpsk', hdx, transfer)
        image = contract('rpsl,pslm->rpsm', x, dense_kernel) + contract('rpsk,pslk->rpsl', zx, leaf_basis)
        dimage = (contract('rpsl,pslm->rpsm', x, dense_deriv) + contract('rpsl,pslm->rpsm', dx, dense_kernel)
                  + contract('rpsk,pslk->rpsl', zdx, leaf_basis))
        x_next = x + relax_step * (rhs - noise_level * x - image)
        dx = dx - relax_step * (noise_level * dx + dimage)
        x = x_next
    return x.reshape(RHS, PARENTS, PTS_PAR), dx.reshape(RHS, PARENTS, PTS_PAR)
```

```python
import functools

import jax
import jax.numpy as jnp
from jax import lax
from jax.experimental import pallas as pl
from jax.experimental.pallas import tpu as pltpu
from jax.sharding import PartitionSpec as P

ITERS = 2
relax_step = 0.3
noise_level = 1.0
keep = 1.0 - relax_step * noise_level


GRANT = 24 * 1024 * 1024

f32 = jnp.float32
bf16 = jnp.bfloat16


def halves(value):
    high = value.astype(bf16)
    return high, (value - high.astype(f32)).astype(bf16)


def one_pass(left, right, contract):
    return lax.dot_general(left, right, (contract, ((), ())), preferred_element_type=f32)


def mm(left, right, contract=((1,), (0,))):
    return (
        one_pass(left[0], right[0], contract)
        + one_pass(left[0], right[1], contract)
        + one_pass(left[1], right[0], contract)
    )


def mm_t(left, right):
    return mm(left, right, ((1,), (1,)))


def rows_of(pair, start, size):
    return tuple(part[start : start + size] for part in pair)


VMEM = pl.BlockSpec(memory_space=pltpu.VMEM)
SMEM = pl.BlockSpec(memory_space=pltpu.SMEM)


def call(kernel, name, inputs, outputs, flops, scratch=(), scalars=0):
    specs = [SMEM] * scalars + [VMEM] * (len(inputs) - scalars)
    moved = sum(4 * item.size for item in inputs)
    return pl.pallas_call(
        kernel,
        name=name,
        in_specs=specs,
        out_specs=tuple(VMEM for _ in outputs),
        out_shape=tuple(jax.ShapeDtypeStruct(shape, f32) for shape in outputs),
        scratch_shapes=list(scratch),
        compiler_params=pltpu.CompilerParams(vmem_limit_bytes=GRANT),
        cost_estimate=pl.CostEstimate(flops=3 * flops, bytes_accessed=moved, transcendentals=0),
    )(*inputs)


def send_quarters(term, count, outs):
    me = lax.axis_index("sib")
    rhs = term.shape[0] // 2
    part = rhs // count
    for o, out in enumerate(outs):
        row = pl.multiple_of(lax.rem(me - o + count, count) * part, part)
        out[:part] = term[pl.ds(row, part)]
        out[part:] = term[pl.ds(pl.multiple_of(rhs + row, part), part)]


def start_kernel(count, x_ref, dx_ref, basis_ref, trans_ref, xs_ref, ab_ref, *rest):
    outs, term = rest[:count], rest[count]
    rhs = x_ref.shape[0]
    xs_ref[:rhs] = x_ref[:, 0, :]
    xs_ref[rhs:] = dx_ref[:, 0, :]
    ab = mm(halves(xs_ref[...]), halves(basis_ref[0, 0]))
    ab_ref[...] = ab
    term[...] = mm(halves(ab), halves(trans_ref[0, 0]))
    send_quarters(term, count, outs)


def local_kernel(xs_ref, dense_ref, deriv_ref, base_ref):
    rhs = xs_ref.shape[0] // 2
    xs = xs_ref[...]
    pair = halves(xs)
    image = mm(pair, halves(dense_ref[0, 0]))
    extra = mm(rows_of(pair, 0, rhs), halves(deriv_ref[0, 0]))
    base_ref[:rhs] = keep * xs[:rhs] - relax_step * image[:rhs]
    base_ref[rhs:] = keep * xs[rhs:] - relax_step * (image[rhs:] + extra)


def sum_kernel(*refs):
    total = refs[0][...]
    for ref in refs[1:-1]:
        total = total + ref[...]
    refs[-1][...] = total


def parent_kernel_body(wide, partners_ref, kern_ref, deriv_ref, *rest):
    pieces, out, held = rest[:wide], rest[wide], rest[wide + 1]
    me = lax.axis_index("wide")
    twin = me + 1 - 2 * lax.rem(me, 2)
    for j in range(wide):
        held[j] = pieces[j][...]
    chosen = []
    for k in range(partners_ref.shape[1]):
        who = partners_ref[0, k]
        other = lax.rem(who + me, 2)
        origin = jnp.where(other == 0, me, twin)
        slot = other * (wide // 2) + lax.div(lax.rem(who - origin + wide, wide), 2)
        chosen.append(held[slot])
    part = out.shape[0] // 2
    pair = halves(jnp.concatenate(chosen, axis=1))
    depth = pair[0].shape[1]
    kern = halves(kern_ref[0].reshape(depth, -1))
    deriv = halves(deriv_ref[0].reshape(depth, -1))
    field = mm(pair, kern)
    out[:part] = field[:part]
    out[part:] = field[part:] + mm(rows_of(pair, 0, part), deriv)


def sibling_body(count, kern_ref, deriv_ref, *rest):
    pieces, out = rest[:-1], rest[-1]
    rhs = out.shape[0] // 2
    total = None
    extra = None
    for o in range(count - 1):
        pair = halves(pieces[o][...])
        term = mm(pair, halves(kern_ref[0, 0, o]))
        more = mm(rows_of(pair, 0, rhs), halves(deriv_ref[0, 0, o]))
        total = term if total is None else total + term
        extra = more if extra is None else extra + more
    out[:rhs] = total[:rhs]
    out[rhs:] = total[rhs:] + extra


def order_body(count, order_ref, *rest):
    pieces, out = rest[:-1], rest[-1]
    me = lax.axis_index("sib")
    rows = pieces[0].shape[-1]
    order = order_ref[...]
    place = lax.broadcasted_iota(jnp.int32, (rows, order.shape[1]), 0)
    total = None
    for o in range(count):
        source = lax.rem(me + o, count) * rows
        pick = (place == order - source).astype(f32).astype(bf16)
        value = pieces[o][:, 0, :]
        high = value.astype(bf16)
        rest_1 = value - high.astype(f32)
        middle = rest_1.astype(bf16)
        low = (rest_1 - middle.astype(f32)).astype(bf16)
        for limb in (high, middle, low):
            term = one_pass(limb, pick, ((1,), (0,)))
            total = term if total is None else total + term
    out[...] = total


def collect(count, pieces, whole):
    me = lax.axis_index("sib")
    rhs = whole.shape[0] // 2
    part = rhs // count
    for o in range(count):
        row = pl.multiple_of(lax.rem(me + o, count) * part, part)
        whole[pl.ds(row, part)] = pieces[o][:part]
        whole[pl.ds(pl.multiple_of(rhs + row, part), part)] = pieces[o][part:]


def updated(whole, basis, trans, near_ref, base_ref, right_ref):
    rhs = right_ref.shape[0]
    field = near_ref[...] + mm_t(halves(whole[...]), trans)
    new = base_ref[...] - relax_step * mm_t(halves(field), basis)
    return new[:rhs] + relax_step * right_ref[...], new[rhs:]


def step_body(count, basis_ref, trans_ref, near_ref, base_ref, right_ref, *rest):
    pieces, rest = rest[:count], rest[count:]
    xs_ref, ab_ref = rest[:2]
    outs, whole, term = rest[2 : 2 + count], rest[2 + count], rest[3 + count]
    rhs = right_ref.shape[0]
    collect(count, pieces, whole)
    basis = halves(basis_ref[0, 0])
    trans = halves(trans_ref[0, 0])
    x, dx = updated(whole, basis, trans, near_ref, base_ref, right_ref)
    xs_ref[:rhs] = x
    xs_ref[rhs:] = dx
    ab = mm(halves(xs_ref[...]), basis)
    ab_ref[...] = ab
    term[...] = mm(halves(ab), trans)
    send_quarters(term, count, outs)


def final_body(count, basis_ref, trans_ref, near_ref, base_ref, right_ref, *rest):
    pieces, (x_out, dx_out, whole) = rest[:count], rest[count:]
    collect(count, pieces, whole)
    basis = halves(basis_ref[0, 0])
    trans = halves(trans_ref[0, 0])
    x, dx = updated(whole, basis, trans, near_ref, base_ref, right_ref)
    x_out[:, 0, :] = x
    dx_out[:, 0, :] = dx


def body(
    right_side,
    tree_order,
    x_start,
    tangent_start,
    dense_kernel,
    dense_deriv,
    leaf_basis,
    transfer,
    sibling_kernel,
    sibling_deriv,
    partner_list,
    parent_kernel,
    parent_deriv,
):
    count = lax.axis_size("sib")
    wide = lax.axis_size("wide")
    rhs = x_start.shape[0]
    leaf = x_start.shape[2]
    rank = leaf_basis.shape[3]
    partners = partner_list.shape[1]
    part = rhs // count
    unit = 2 * rhs * rank * rank

    def sib_from(value, o):
        return lax.ppermute(value, "sib", [(i, (i - o) % count) for i in range(count)])

    def wide_from(value, k):
        return lax.ppermute(value, "wide", [(i, (i - 2 * k) % wide) for i in range(wide)])

    def twin_of(value):
        return lax.ppermute(value, "wide", [(i, i ^ 1) for i in range(wide)])

    quarter = (2 * part, rank)
    both = (2 * rhs, rank)
    points = (2 * rhs, leaf)
    depth = leaf // rank

    xs, ab, *terms = call(
        functools.partial(start_kernel, count),
        "start",
        (x_start, tangent_start, leaf_basis, transfer),
        (points, both) + (quarter,) * count,
        unit * (2 * depth + 2),
        scratch=(pltpu.VMEM(both, f32),),
    )
    right = None
    for step in range(ITERS):
        got_terms = [terms[0]] + [sib_from(terms[o], o) for o in range(1, count)]
        (mine,) = call(sum_kernel, "sum", got_terms, (quarter,), unit // count)
        got_ab = [sib_from(ab, o) for o in range(1, count)]
        if right is None:
            got_right = [right_side] + [sib_from(right_side, o) for o in range(1, count)]
        own = [mine] + [wide_from(mine, k) for k in range(1, wide // 2)]
        twins = [twin_of(item) for item in own]
        (base,) = call(
            local_kernel, "local", (xs, dense_kernel, dense_deriv), (points,), unit * 3 * depth * depth
        )
        (near,) = call(
            functools.partial(sibling_body, count),
            "near",
            [sibling_kernel, sibling_deriv] + got_ab,
            (both,),
            unit * 3 * (count - 1),
        )
        (field,) = call(
            functools.partial(parent_kernel_body, wide),
            "parent",
            [partner_list, parent_kernel, parent_deriv] + own + twins,
            (quarter,),
            unit * 3 * partners // count,
            scratch=(pltpu.VMEM((wide,) + quarter, f32),),
            scalars=1,
        )
        got_field = [field] + [sib_from(field, o) for o in range(1, count)]
        if right is None:
            (right,) = call(
                functools.partial(order_body, count),
                "order",
                [tree_order] + got_right,
                ((rhs, leaf),),
                unit * depth * depth * count,
            )
        known = [leaf_basis, transfer, near, base, right] + got_field
        if step < ITERS - 1:
            xs, ab, *terms = call(
                functools.partial(step_body, count),
                "step",
                known,
                (points, both) + (quarter,) * count,
                unit * (4 * depth + 4),
                scratch=(pltpu.VMEM(both, f32), pltpu.VMEM(both, f32)),
            )
        else:
            x, dx = call(
                functools.partial(final_body, count),
                "final",
                known,
                ((rhs, 1, leaf), (rhs, 1, leaf)),
                unit * (2 * depth + 2),
                scratch=(pltpu.VMEM(both, f32),),
            )
    return x, dx


def solution(mesh):
    placed = (
        P(None, "wide", "sib"),
        P("wide", "sib"),
        P(None, "wide", "sib"),
        P(None, "wide", "sib"),
        P("wide", "sib", None, None),
        P("wide", "sib", None, None),
        P("wide", "sib", None, None),
        P("wide", "sib", None, None),
        P("wide", "sib", None, None, None),
        P("wide", "sib", None, None, None),
        P("wide", None),
        P("wide", None, None, None),
        P("wide", None, None, None),
    )
    return jax.shard_map(
        body,
        mesh=mesh,
        in_specs=placed,
        out_specs=(P(None, "wide", "sib"), P(None, "wide", "sib")),
        check_vma=False,
    )
```

```python
import functools

import jax
import jax.numpy as jnp
from jax import lax
from jax.experimental import pallas as pl
from jax.experimental.pallas import tpu as pltpu
from jax.sharding import PartitionSpec as P

ITERS = 2
relax_step = 0.3
noise_level = 1.0
keep = 1.0 - relax_step * noise_level


GRANT = 24 * 1024 * 1024

f32 = jnp.float32
bf16 = jnp.bfloat16


def halves(value):
    high = value.astype(bf16)
    return high, (value - high.astype(f32)).astype(bf16)


def one_pass(left, right, contract):
    return lax.dot_general(left, right, (contract, ((), ())), preferred_element_type=f32)


def mm(left, right, contract=((1,), (0,))):
    return (
        one_pass(left[0], right[0], contract)
        + one_pass(left[0], right[1], contract)
        + one_pass(left[1], right[0], contract)
    )


def mm_t(left, right):
    return mm(left, right, ((1,), (1,)))


def rows_of(pair, start, size):
    return tuple(part[start : start + size] for part in pair)


VMEM = pl.BlockSpec(memory_space=pltpu.VMEM)
SMEM = pl.BlockSpec(memory_space=pltpu.SMEM)


def call(kernel, name, inputs, outputs, flops, scratch=(), scalars=0):
    specs = [SMEM] * scalars + [VMEM] * (len(inputs) - scalars)
    moved = sum(4 * item.size for item in inputs)
    return pl.pallas_call(
        kernel,
        name=name,
        in_specs=specs,
        out_specs=tuple(VMEM for _ in outputs),
        out_shape=tuple(jax.ShapeDtypeStruct(shape, f32) for shape in outputs),
        scratch_shapes=list(scratch),
        compiler_params=pltpu.CompilerParams(vmem_limit_bytes=GRANT),
        cost_estimate=pl.CostEstimate(flops=3 * flops, bytes_accessed=moved, transcendentals=0),
    )(*inputs)


def peer(o):
    return lax.bitwise_xor(lax.axis_index("sib"), o)


def send_quarters(term, count, outs):
    rhs = term.shape[0] // 2
    part = rhs // count
    for o, out in enumerate(outs):
        row = pl.multiple_of(peer(o) * part, part)
        out[:part] = term[pl.ds(row, part)]
        out[part:] = term[pl.ds(pl.multiple_of(rhs + row, part), part)]


def start_kernel(count, x_ref, dx_ref, basis_ref, trans_ref, xs_ref, ab_ref, *rest):
    outs, term = rest[:count], rest[count]
    rhs = x_ref.shape[0]
    xs_ref[:rhs] = x_ref[:, 0, :]
    xs_ref[rhs:] = dx_ref[:, 0, :]
    ab = mm(halves(xs_ref[...]), halves(basis_ref[0, 0]))
    ab_ref[...] = ab
    term[...] = mm(halves(ab), halves(trans_ref[0, 0]))
    send_quarters(term, count, outs)


def local_kernel(xs_ref, dense_ref, deriv_ref, base_ref):
    rhs = xs_ref.shape[0] // 2
    xs = xs_ref[...]
    pair = halves(xs)
    image = mm(pair, halves(dense_ref[0, 0]))
    extra = mm(rows_of(pair, 0, rhs), halves(deriv_ref[0, 0]))
    base_ref[:rhs] = keep * xs[:rhs] - relax_step * image[:rhs]
    base_ref[rhs:] = keep * xs[rhs:] - relax_step * (image[rhs:] + extra)


def sum_kernel(*refs):
    total = refs[0][...]
    for ref in refs[1:-1]:
        total = total + ref[...]
    refs[-1][...] = total


def parent_kernel_body(wide, partners_ref, kern_ref, deriv_ref, *rest):
    pieces, out, held = rest[:wide], rest[wide], rest[wide + 1]
    me = lax.axis_index("wide")
    for j in range(wide):
        held[j] = pieces[j][...]
    chosen = []
    for k in range(partners_ref.shape[1]):
        apart = lax.bitwise_xor(partners_ref[0, k], me)
        slot = lax.rem(apart, 2) * (wide // 2) + lax.div(apart, 2)
        chosen.append(held[slot])
    part = out.shape[0] // 2
    pair = halves(jnp.concatenate(chosen, axis=1))
    depth = pair[0].shape[1]
    kern = halves(kern_ref[0].reshape(depth, -1))
    deriv = halves(deriv_ref[0].reshape(depth, -1))
    field = mm(pair, kern)
    out[:part] = field[:part]
    out[part:] = field[part:] + mm(rows_of(pair, 0, part), deriv)


def grouped(sizes, refs):
    refs = iter(refs)
    return [[next(refs) for _ in range(size)] for size in sizes]


def sibling_body(sizes, kern_ref, deriv_ref, *rest):
    pieces, out = grouped(sizes, rest[:-1]), rest[-1]
    count = len(sizes) + 1
    me = lax.axis_index("sib")
    rhs = out.shape[0] // 2
    total = None
    extra = None
    for o in range(1, count):
        parts = [ref[...] for ref in pieces[o - 1]]
        value = parts[0] if len(parts) == 1 else jnp.concatenate(parts, axis=0)
        slot = lax.rem(peer(o) - me - 1 + count, count)
        pair = halves(value)
        term = mm(pair, halves(kern_ref[0, 0, slot]))
        more = mm(rows_of(pair, 0, rhs), halves(deriv_ref[0, 0, slot]))
        total = term if total is None else total + term
        extra = more if extra is None else extra + more
    out[:rhs] = total[:rhs]
    out[rhs:] = total[rhs:] + extra


def order_body(sizes, order_ref, *rest):
    pieces, (out, value, pick) = grouped(sizes, rest[:-3]), rest[-3:]
    count = len(sizes)
    rhs, columns = out.shape
    rows = pieces[0][0].shape[-1]
    place = lax.broadcasted_iota(jnp.int32, (rows, columns), 0)
    for o in range(count):
        span = pl.ds(o * rows, rows)
        pick[span] = jnp.where(place == order_ref[...] - peer(o) * rows, 1.0, 0.0).astype(bf16)
        at = 0
        for ref in pieces[o]:
            high, low = halves(ref[:, 0, :])
            value[pl.ds(at, ref.shape[0]), span] = high
            value[pl.ds(rhs + at, ref.shape[0]), span] = low
            at += ref.shape[0]
    both = one_pass(value[...], pick[...], ((1,), (0,)))
    out[...] = both[:rhs] + both[rhs:]


def collect(count, pieces, whole):
    rhs = whole.shape[0] // 2
    part = rhs // count
    for o in range(count):
        row = pl.multiple_of(peer(o) * part, part)
        whole[pl.ds(row, part)] = pieces[o][:part]
        whole[pl.ds(pl.multiple_of(rhs + row, part), part)] = pieces[o][part:]


def updated(whole, basis, trans, near_ref, base_ref, right_ref):
    rhs = right_ref.shape[0]
    field = near_ref[...] + mm_t(halves(whole[...]), trans)
    new = base_ref[...] - relax_step * mm_t(halves(field), basis)
    return new[:rhs] + relax_step * right_ref[...], new[rhs:]


def step_body(count, basis_ref, trans_ref, near_ref, base_ref, right_ref, *rest):
    pieces, rest = rest[:count], rest[count:]
    xs_ref, ab_ref = rest[:2]
    outs, whole, term = rest[2 : 2 + count], rest[2 + count], rest[3 + count]
    rhs = right_ref.shape[0]
    collect(count, pieces, whole)
    basis = halves(basis_ref[0, 0])
    trans = halves(trans_ref[0, 0])
    x, dx = updated(whole, basis, trans, near_ref, base_ref, right_ref)
    xs_ref[:rhs] = x
    xs_ref[rhs:] = dx
    ab = mm(halves(xs_ref[...]), basis)
    ab_ref[...] = ab
    term[...] = mm(halves(ab), trans)
    send_quarters(term, count, outs)


def final_body(count, basis_ref, trans_ref, near_ref, base_ref, right_ref, *rest):
    pieces, (x_out, dx_out, whole) = rest[:count], rest[count:]
    collect(count, pieces, whole)
    basis = halves(basis_ref[0, 0])
    trans = halves(trans_ref[0, 0])
    x, dx = updated(whole, basis, trans, near_ref, base_ref, right_ref)
    x_out[:, 0, :] = x
    dx_out[:, 0, :] = dx


def body(
    right_side,
    tree_order,
    x_start,
    tangent_start,
    dense_kernel,
    dense_deriv,
    leaf_basis,
    transfer,
    sibling_kernel,
    sibling_deriv,
    partner_list,
    parent_kernel,
    parent_deriv,
):
    count = lax.axis_size("sib")
    wide = lax.axis_size("wide")
    rhs = x_start.shape[0]
    leaf = x_start.shape[2]
    rank = leaf_basis.shape[3]
    partners = partner_list.shape[1]
    part = rhs // count
    unit = 2 * rhs * rank * rank

    def sib_from(value, o):
        return lax.ppermute(value, "sib", [(i, i ^ o) for i in range(count)])

    def wide_from(value, k):
        return lax.ppermute(value, "wide", [(i, i ^ k) for i in range(wide)])

    def exchange(value):
        if count != 4:
            return [[value]] + [[sib_from(value, o)] for o in range(1, count)]
        half = value.shape[0] // 2
        first, second = sib_from(value, 1), sib_from(value, 2)
        corner = [sib_from(first[:half], 2), sib_from(second[half:], 1)]
        return [[value], [first], [second], corner]

    def flat(groups):
        return [item for group in groups for item in group], [len(group) for group in groups]

    quarter = (2 * part, rank)
    both = (2 * rhs, rank)
    points = (2 * rhs, leaf)
    depth = leaf // rank

    got_right, right_sizes = flat(exchange(right_side))
    xs, ab, *terms = call(
        functools.partial(start_kernel, count),
        "start",
        (x_start, tangent_start, leaf_basis, transfer),
        (points, both) + (quarter,) * count,
        unit * (2 * depth + 2),
        scratch=(pltpu.VMEM(both, f32),),
    )
    right = None
    for step in range(ITERS):
        got_terms = [terms[0]] + [sib_from(terms[o], o) for o in range(1, count)]
        (mine,) = call(sum_kernel, "sum", got_terms, (quarter,), unit // count)
        mine, ab = lax.optimization_barrier((mine, ab))
        own = [mine] + [wide_from(mine, 2 * k) for k in range(1, wide // 2)]
        got_ab, ab_sizes = flat(exchange(ab)[1:])
        twins = [wide_from(item, 1) for item in own]
        (base,) = call(
            local_kernel, "local", (xs, dense_kernel, dense_deriv), (points,), unit * 3 * depth * depth
        )
        if right is None:
            (right,) = call(
                functools.partial(order_body, right_sizes),
                "order",
                [tree_order] + got_right,
                ((rhs, leaf),),
                unit * depth * depth * count,
                scratch=(pltpu.VMEM((2 * rhs, count * leaf), bf16), pltpu.VMEM((count * leaf, leaf), bf16)),
            )
        (near,) = call(
            functools.partial(sibling_body, ab_sizes),
            "near",
            [sibling_kernel, sibling_deriv] + got_ab,
            (both,),
            unit * 3 * (count - 1),
        )
        (field,) = call(
            functools.partial(parent_kernel_body, wide),
            "parent",
            [partner_list, parent_kernel, parent_deriv] + own + twins,
            (quarter,),
            unit * 3 * partners // count,
            scratch=(pltpu.VMEM((wide,) + quarter, f32),),
            scalars=1,
        )
        got_field = [field] + [sib_from(field, o) for o in range(1, count)]
        known = [leaf_basis, transfer, near, base, right] + got_field
        if step < ITERS - 1:
            xs, ab, *terms = call(
                functools.partial(step_body, count),
                "step",
                known,
                (points, both) + (quarter,) * count,
                unit * (4 * depth + 4),
                scratch=(pltpu.VMEM(both, f32), pltpu.VMEM(both, f32)),
            )
        else:
            x, dx = call(
                functools.partial(final_body, count),
                "final",
                known,
                ((rhs, 1, leaf), (rhs, 1, leaf)),
                unit * (2 * depth + 2),
                scratch=(pltpu.VMEM(both, f32),),
            )
    return x, dx


def solution(mesh):
    placed = (
        P(None, "wide", "sib"),
        P("wide", "sib"),
        P(None, "wide", "sib"),
        P(None, "wide", "sib"),
        P("wide", "sib", None, None),
        P("wide", "sib", None, None),
        P("wide", "sib", None, None),
        P("wide", "sib", None, None),
        P("wide", "sib", None, None, None),
        P("wide", "sib", None, None, None),
        P("wide", None),
        P("wide", None, None, None),
        P("wide", None, None, None),
    )
    return jax.shard_map(
        body,
        mesh=mesh,
        in_specs=placed,
        out_specs=(P(None, "wide", "sib"), P(None, "wide", "sib")),
        check_vma=False,
    )
```

```python
import functools

import jax
import jax.numpy as jnp
from jax import lax
from jax.experimental import pallas as pl
from jax.experimental.pallas import tpu as pltpu
from jax.sharding import PartitionSpec as P


ITERS = 2
relax_step = 0.3
noise_level = 1.0
keep = 1.0 - relax_step * noise_level


GRANT = 24 * 1024 * 1024
LARGE = 61 * 1024 * 1024

f32 = jnp.float32
bf16 = jnp.bfloat16


def halves(value):
    high = value.astype(bf16)
    return high, (value - high.astype(f32)).astype(bf16)


def one_pass(left, right, contract):
    return lax.dot_general(left, right, (contract, ((), ())), preferred_element_type=f32)


def mm(left, right, contract=((1,), (0,))):
    return (
        one_pass(left[0], right[0], contract)
        + one_pass(left[0], right[1], contract)
        + one_pass(left[1], right[0], contract)
    )


def mm_t(left, right):
    return mm(left, right, ((1,), (1,)))


def rows_of(pair, start, size):
    return tuple(part[start : start + size] for part in pair)


VMEM = pl.BlockSpec(memory_space=pltpu.VMEM)
SMEM = pl.BlockSpec(memory_space=pltpu.SMEM)
HBM = pl.BlockSpec(memory_space=pltpu.HBM)


def call(kernel, inputs, outputs, flops, scratch=(), scalars=0, specs=None, kind=f32, grant=GRANT):
    if specs is None:
        specs = [SMEM] * scalars + [VMEM] * (len(inputs) - scalars)
    moved = sum(4 * item.size for item in inputs)
    return pl.pallas_call(
        kernel,
        in_specs=specs,
        out_specs=tuple(VMEM for _ in outputs),
        out_shape=tuple(jax.ShapeDtypeStruct(shape, kind) for shape in outputs),
        scratch_shapes=list(scratch),
        compiler_params=pltpu.CompilerParams(vmem_limit_bytes=grant),
        cost_estimate=pl.CostEstimate(flops=3 * flops, bytes_accessed=moved, transcendentals=0),
    )(*inputs)


def peer(o):
    return lax.bitwise_xor(lax.axis_index("sib"), o)


def send_quarters(term, count, outs):
    rhs = term.shape[0] // 2
    part = rhs // count
    for o, out in enumerate(outs):
        row = pl.multiple_of(peer(o) * part, part)
        out[:part] = term[pl.ds(row, part)]
        out[part:] = term[pl.ds(pl.multiple_of(rhs + row, part), part)]


def start_kernel(count, *refs):
    loads, (xs_ref, ab_ref, *outs) = refs[:4], refs[4 : 6 + count]
    term, *held, done = refs[6 + count :]
    copies = [pltpu.make_async_copy(*ends, done.at[k]) for k, ends in enumerate(zip(loads, held))]
    for copy in copies:
        copy.start()
    for copy in copies:
        copy.wait()
    x_ref, dx_ref, basis_ref, trans_ref = held
    rhs = x_ref.shape[0]
    xs_ref[:rhs] = x_ref[:, 0, :]
    xs_ref[rhs:] = dx_ref[:, 0, :]
    ab = mm(halves(xs_ref[...]), halves(basis_ref[0, 0]))
    ab_ref[...] = ab
    term[...] = mm(halves(ab), halves(trans_ref[0, 0]))
    send_quarters(term, count, outs)


def local_kernel(xs_ref, dense_ref, deriv_ref, base_ref):
    rhs = xs_ref.shape[0] // 2
    xs = xs_ref[...]
    pair = halves(xs)
    image = mm(pair, halves(dense_ref[0, 0]))
    extra = mm(rows_of(pair, 0, rhs), halves(deriv_ref[0, 0]))
    base_ref[:rhs] = keep * xs[:rhs] - relax_step * image[:rhs]
    base_ref[rhs:] = keep * xs[rhs:] - relax_step * (image[rhs:] + extra)


def sum_kernel(*refs):
    total = refs[0][...]
    for ref in refs[1:-1]:
        total = total + ref[...]
    refs[-1][...] = total


def parent_kernel_body(wide, partners_ref, kern_ref, deriv_ref, *rest):
    *pieces, out, held = rest
    me = lax.axis_index("wide")
    at = 0
    for ref in pieces:
        for row in range(0, ref.shape[0], out.shape[0]):
            held[at] = ref[row : row + out.shape[0]]
            at += 1
    chosen = []
    for k in range(partners_ref.shape[1]):
        apart = lax.bitwise_xor(partners_ref[0, k], me)
        slot = lax.rem(apart, 2) * (wide // 2) + lax.div(apart, 2)
        chosen.append(held[slot])
    part = out.shape[0] // 2
    pair = halves(jnp.concatenate(chosen, axis=1))
    depth = pair[0].shape[1]
    kern = halves(kern_ref[0].reshape(depth, -1))
    deriv = halves(deriv_ref[0].reshape(depth, -1))
    field = mm(pair, kern)
    out[:part] = field[:part]
    out[part:] = field[part:] + mm(rows_of(pair, 0, part), deriv)


def grouped(sizes, refs):
    refs = iter(refs)
    return [[next(refs) for _ in range(size)] for size in sizes]


def sibling_body(sizes, kern_ref, deriv_ref, *rest):
    pieces, out = grouped(sizes, rest[:-1]), rest[-1]
    count = len(sizes) + 1
    me = lax.axis_index("sib")
    rhs = out.shape[0] // 2
    total = None
    extra = None
    for o in range(1, count):
        parts = [ref[...] for ref in pieces[o - 1]]
        value = parts[0] if len(parts) == 1 else jnp.concatenate(parts, axis=0)
        slot = lax.rem(peer(o) - me - 1 + count, count)
        pair = halves(value)
        term = mm(pair, halves(kern_ref[0, 0, slot]))
        more = mm(rows_of(pair, 0, rhs), halves(deriv_ref[0, 0, slot]))
        total = term if total is None else total + term
        extra = more if extra is None else extra + more
    out[:rhs] = total[:rhs]
    out[rhs:] = total[rhs:] + extra


def pick_body(count, order_ref, pick):
    columns = order_ref.shape[1]
    rows = pick.shape[0] // count
    chunk = 16
    place = lax.broadcasted_iota(jnp.int32, (chunk, columns), 0)
    for o in range(count):
        wanted = jnp.broadcast_to(order_ref[...] - peer(o) * rows, (chunk, columns)) - place
        for at in range(0, rows, chunk):
            pick[pl.ds(o * rows + at, chunk)] = jnp.where(wanted == at, 1.0, 0.0).astype(bf16)


def order_body(pick, *rest):
    pieces, (out, value) = rest[:-2], rest[-2:]
    rhs = out.shape[0]
    rows = pieces[0].shape[-1]
    for o, ref in enumerate(pieces):
        value[:, o * rows : (o + 1) * rows] = ref[:, 0, :]
    both = one_pass(jnp.concatenate(halves(value[...]), axis=0), pick[...], ((1,), (0,)))
    out[...] = both[:rhs] + both[rhs:]


def collect(count, pieces, whole):
    rhs = whole.shape[0] // 2
    part = rhs // count
    for o in range(count):
        row = pl.multiple_of(peer(o) * part, part)
        whole[pl.ds(row, part)] = pieces[o][:part]
        whole[pl.ds(pl.multiple_of(rhs + row, part), part)] = pieces[o][part:]


def weights_body(basis_ref, trans_ref, lift_ref, again_ref, term_ref):
    basis = halves(basis_ref[0, 0])
    trans = halves(trans_ref[0, 0])
    lift = mm(basis, trans)
    lift_ref[...] = lift
    again = mm(halves(lift), basis, ((0,), (0,)))
    again_ref[...] = again
    term_ref[...] = mm(halves(again), trans)


def before_body(last, basis_ref, trans_ref, near_ref, base_ref, right_ref, *outs):
    rhs = right_ref.shape[0]
    new_ref = outs[0]
    basis = halves(basis_ref[0, 0])
    new_ref[...] = base_ref[...] - relax_step * mm_t(halves(near_ref[...]), basis)
    new_ref[:rhs] = new_ref[:rhs] + relax_step * right_ref[...]
    if not last:
        ab = mm(halves(new_ref[...]), basis)
        outs[1][...] = ab
        outs[2][...] = mm(halves(ab), halves(trans_ref[0, 0]))


def terms_body(count, weight_ref, before_ref, *rest):
    pieces, rest = rest[:count], rest[count:]
    outs, (whole, term) = rest[:count], rest[count:]
    collect(count, pieces, whole)
    term[...] = before_ref[...] - relax_step * mm(halves(whole[...]), halves(weight_ref[...]))
    send_quarters(term, count, outs)


def coeffs_body(count, weight_ref, before_ref, *rest):
    pieces, (out, whole) = rest[:count], rest[count:]
    collect(count, pieces, whole)
    out[...] = before_ref[...] - relax_step * mm(halves(whole[...]), halves(weight_ref[...]))


def points_body(count, last, lift_ref, new_ref, *rest):
    pieces, (*outs, whole) = rest[:count], rest[count:]
    collect(count, pieces, whole)
    new = new_ref[...] - relax_step * mm_t(halves(whole[...]), halves(lift_ref[...]))
    if last:
        rhs = new.shape[0] // 2
        outs[0][:, 0, :] = new[:rhs]
        outs[1][:, 0, :] = new[rhs:]
    else:
        outs[0][...] = new


def join_body(*refs):
    for k, ref in enumerate(refs[:-1]):
        refs[-1][k * ref.shape[0] : (k + 1) * ref.shape[0]] = ref[...]


def body(
    right_side,
    tree_order,
    x_start,
    tangent_start,
    dense_kernel,
    dense_deriv,
    leaf_basis,
    transfer,
    sibling_kernel,
    sibling_deriv,
    partner_list,
    parent_kernel,
    parent_deriv,
):
    count = lax.axis_size("sib")
    wide = lax.axis_size("wide")
    rhs = x_start.shape[0]
    leaf = x_start.shape[2]
    rank = leaf_basis.shape[3]
    partners = partner_list.shape[1]
    part = rhs // count
    unit = 2 * rhs * rank * rank

    def sib_from(value, o):
        return lax.ppermute(value, "sib", [(i, i ^ o) for i in range(count)])

    def wide_from(value, k):
        return lax.ppermute(value, "wide", [(i, i ^ k) for i in range(wide)])

    quarter = (2 * part, rank)
    both = (2 * rhs, rank)
    points = (2 * rhs, leaf)
    depth = leaf // rank

    def siblings(values):
        got = {}
        for o in reversed(range(1, count)):
            got[o] = sib_from(values[o], o)
        return [got[o] for o in range(1, count)]

    loaded = (x_start, tangent_start, leaf_basis, transfer)
    xs, ab, *terms = call(
        functools.partial(start_kernel, count),
        loaded,
        (points, both) + (quarter,) * count,
        unit * (2 * depth + 2),
        scratch=[pltpu.VMEM(both, f32)]
        + [pltpu.VMEM(item.shape, f32) for item in loaded]
        + [pltpu.SemaphoreType.DMA((len(loaded),))],
        specs=[HBM] * len(loaded),
        grant=LARGE,
    )
    got_right = [right_side] + siblings([right_side] * count)
    lift, again_weight, term_weight = call(
        weights_body,
        (leaf_basis, transfer),
        ((leaf, rank), (rank, rank), (rank, rank)),
        unit * 4 * depth,
    )
    (pick,) = call(
        functools.partial(pick_body, count),
        (tree_order,),
        ((count * leaf, leaf),),
        unit * depth,
        kind=bf16,
    )
    right = None
    for step in range(ITERS):
        last = step == ITERS - 1
        got_terms = [terms[0]] + siblings(terms)
        (mine,) = call(sum_kernel, got_terms, (quarter,), unit // count)
        away = {}
        for k in reversed(range(1, wide // 2)):
            away[k] = wide_from(mine, 2 * k)
        away = [away[k] for k in range(1, wide // 2)]
        twin = wide_from(mine, 1)
        if not last:
            mine, ab = lax.optimization_barrier((mine, ab))
        got_ab = siblings([ab] * count)
        (joined,) = call(join_body, away, (((wide // 2 - 1) * 2 * part, rank),), unit // count)
        twins = wide_from(joined, 1)
        (base,) = call(
            local_kernel, (xs, dense_kernel, dense_deriv), (points,), unit * 3 * depth * depth
        )
        if right is None:
            (right,) = call(
                order_body,
                [pick] + got_right,
                ((rhs, leaf),),
                unit * depth * depth * count,
                scratch=(pltpu.VMEM((rhs, count * leaf), f32),),
            )
        (near,) = call(
            functools.partial(sibling_body, [1] * (count - 1)),
            [sibling_kernel, sibling_deriv] + got_ab,
            (both,),
            unit * 3 * (count - 1),
        )
        before = call(
            functools.partial(before_body, last),
            [leaf_basis, transfer, near, base, right],
            (points,) if last else (points, both, both),
            unit * 4 * depth,
        )
        (field,) = call(
            functools.partial(parent_kernel_body, wide),
            [partner_list, parent_kernel, parent_deriv, mine, joined, twin, twins],
            (quarter,),
            unit * 3 * partners // count,
            scratch=(pltpu.VMEM((wide,) + quarter, f32),),
            scalars=1,
        )
        got_field = [field] + siblings([field] * count)
        whole = pltpu.VMEM(both, f32)
        if not last:
            terms = call(
                functools.partial(terms_body, count),
                [term_weight, before[2]] + got_field,
                (quarter,) * count,
                unit * 2,
                scratch=(whole, whole),
            )
            (ab,) = call(
                functools.partial(coeffs_body, count),
                [again_weight, before[1]] + got_field,
                (both,),
                unit * 2,
                scratch=(whole,),
            )
        shape = ((rhs, 1, leaf),) * 2 if last else (points,)
        xs, *more = call(
            functools.partial(points_body, count, last),
            [lift, before[0]] + got_field,
            shape,
            unit * 2 * depth,
            scratch=(whole,),
        )
    return xs, more[0]


def solution(mesh):
    placed = (
        P(None, "wide", "sib"),
        P("wide", "sib"),
        P(None, "wide", "sib"),
        P(None, "wide", "sib"),
        P("wide", "sib", None, None),
        P("wide", "sib", None, None),
        P("wide", "sib", None, None),
        P("wide", "sib", None, None),
        P("wide", "sib", None, None, None),
        P("wide", "sib", None, None, None),
        P("wide", None),
        P("wide", None, None, None),
        P("wide", None, None, None),
    )
    return jax.shard_map(
        body,
        mesh=mesh,
        in_specs=placed,
        out_specs=(P(None, "wide", "sib"), P(None, "wide", "sib")),
        check_vma=False,
    )
```

```python
import functools

import jax
import jax.numpy as jnp
from jax import lax
from jax.experimental import pallas as pl
from jax.experimental.pallas import tpu as pltpu
from jax.sharding import PartitionSpec as P


ITERS = 2
relax_step = 0.3
noise_level = 1.0
keep = 1.0 - relax_step * noise_level


GRANT = 24 * 1024 * 1024
LARGE = 53 * 1024 * 1024

f32 = jnp.float32
bf16 = jnp.bfloat16


def halves(value):
    high = value.astype(bf16)
    return high, (value - high.astype(f32)).astype(bf16)


def one_pass(left, right, contract):
    return lax.dot_general(left, right, (contract, ((), ())), preferred_element_type=f32)


def mm(left, right, contract=((1,), (0,))):
    return (
        one_pass(left[0], right[0], contract)
        + one_pass(left[0], right[1], contract)
        + one_pass(left[1], right[0], contract)
    )


def mm_t(left, right):
    return mm(left, right, ((1,), (1,)))


def rows_of(pair, start, size):
    return tuple(part[start : start + size] for part in pair)


VMEM = pl.BlockSpec(memory_space=pltpu.VMEM)
SMEM = pl.BlockSpec(memory_space=pltpu.SMEM)
HBM = pl.BlockSpec(memory_space=pltpu.HBM)


def call(kernel, inputs, outputs, flops, scratch=(), scalars=0, specs=None, kind=f32, grant=GRANT):
    if specs is None:
        specs = [SMEM] * scalars + [VMEM] * (len(inputs) - scalars)
    moved = sum(4 * item.size for item in inputs)
    return pl.pallas_call(
        kernel,
        in_specs=specs,
        out_specs=tuple(VMEM for _ in outputs),
        out_shape=tuple(jax.ShapeDtypeStruct(shape, kind) for shape in outputs),
        scratch_shapes=list(scratch),
        compiler_params=pltpu.CompilerParams(vmem_limit_bytes=grant),
        cost_estimate=pl.CostEstimate(flops=3 * flops, bytes_accessed=moved, transcendentals=0),
    )(*inputs)


def peer(o):
    return lax.bitwise_xor(lax.axis_index("sib"), o)


def send_quarters(term, count, outs):
    rhs = term.shape[0] // 2
    part = rhs // count
    for o, out in enumerate(outs):
        row = pl.multiple_of(peer(o) * part, part)
        out[:part] = term[pl.ds(row, part)]
        out[part:] = term[pl.ds(pl.multiple_of(rhs + row, part), part)]


def start_kernel(count, *refs):
    loads, (basis_out, trans_out, xs_ref, ab_ref, *outs) = refs[:4], refs[4 : 8 + count]
    term, *held, done = refs[8 + count :]
    copies = [pltpu.make_async_copy(*ends, done.at[k]) for k, ends in enumerate(zip(loads, held))]
    for copy in copies:
        copy.start()
    for copy in copies:
        copy.wait()
    x_ref, dx_ref, basis_ref, trans_ref = held
    rhs = x_ref.shape[0]
    xs_ref[:rhs] = x_ref[:, 0, :]
    xs_ref[rhs:] = dx_ref[:, 0, :]
    ab = mm(halves(xs_ref[...]), halves(basis_ref[0, 0]))
    ab_ref[...] = ab
    term[...] = mm(halves(ab), halves(trans_ref[0, 0]))
    send_quarters(term, count, outs)
    basis_out[...] = basis_ref[...]
    trans_out[...] = trans_ref[...]


def local_kernel(xs_ref, dense_ref, deriv_ref, base_ref):
    rhs = xs_ref.shape[0] // 2
    xs = xs_ref[...]
    pair = halves(xs)
    image = mm(pair, halves(dense_ref[0, 0]))
    extra = mm(rows_of(pair, 0, rhs), halves(deriv_ref[0, 0]))
    base_ref[:rhs] = keep * xs[:rhs] - relax_step * image[:rhs]
    base_ref[rhs:] = keep * xs[rhs:] - relax_step * (image[rhs:] + extra)


def sum_kernel(*refs):
    total = refs[0][...]
    for ref in refs[1:-1]:
        total = total + ref[...]
    refs[-1][...] = total


def parent_kernel_body(wide, partners_ref, kern_ref, deriv_ref, *rest):
    *pieces, out, held = rest
    me = lax.axis_index("wide")
    at = 0
    for ref in pieces:
        for row in range(0, ref.shape[0], out.shape[0]):
            held[at] = ref[row : row + out.shape[0]]
            at += 1
    apart = lax.bitwise_xor(partners_ref[...], jnp.full(partners_ref.shape, me, jnp.int32))
    slots = (apart & 1) * (wide // 2) + (apart >> 1)
    chosen = []
    for k in range(partners_ref.shape[1]):
        slot = jnp.broadcast_to(slots[:, k : k + 1], out.shape)
        value = held[0]
        for j in range(1, wide):
            value = jnp.where(slot == j, held[j], value)
        chosen.append(value)
    part = out.shape[0] // 2
    pair = halves(jnp.concatenate(chosen, axis=1))
    depth = pair[0].shape[1]
    kern = halves(kern_ref[0].reshape(depth, -1))
    deriv = halves(deriv_ref[0].reshape(depth, -1))
    field = mm(pair, kern)
    out[:part] = field[:part]
    out[part:] = field[part:] + mm(rows_of(pair, 0, part), deriv)


def grouped(sizes, refs):
    refs = iter(refs)
    return [[next(refs) for _ in range(size)] for size in sizes]


def sibling_body(sizes, kern_ref, deriv_ref, *rest):
    pieces, out = grouped(sizes, rest[:-1]), rest[-1]
    count = len(sizes) + 1
    me = lax.axis_index("sib")
    rhs = out.shape[0] // 2
    total = None
    extra = None
    for o in range(1, count):
        parts = [ref[:rhs] if len(pieces[o - 1]) > 1 else ref[...] for ref in pieces[o - 1]]
        value = parts[0] if len(parts) == 1 else jnp.concatenate(parts, axis=0)
        slot = lax.rem(peer(o) - me - 1 + count, count)
        pair = halves(value)
        term = mm(pair, halves(kern_ref[0, 0, slot]))
        more = mm(rows_of(pair, 0, rhs), halves(deriv_ref[0, 0, slot]))
        total = term if total is None else total + term
        extra = more if extra is None else extra + more
    out[:rhs] = total[:rhs]
    out[rhs:] = total[rhs:] + extra


def pick_body(count, order_ref, pick):
    columns = order_ref.shape[1]
    rows = pick.shape[0] // count
    chunk = 16
    place = lax.broadcasted_iota(jnp.int32, (chunk, columns), 0)
    for o in range(count):
        wanted = jnp.broadcast_to(order_ref[...] - peer(o) * rows, (chunk, columns)) - place
        for at in range(0, rows, chunk):
            pick[pl.ds(o * rows + at, chunk)] = jnp.where(wanted == at, 1.0, 0.0).astype(bf16)


def pack_body(right_1_ref, right_2_ref, ab_1_ref, ab_2_ref, out_1, out_2, held):
    rhs = right_1_ref.shape[0]
    half = rhs // 2
    rank = out_1.shape[1]
    for right_ref, ab_ref, out, row in ((right_1_ref, ab_1_ref, out_1, 0), (right_2_ref, ab_2_ref, out_2, half)):
        out[:rhs] = ab_ref[2 * row : 2 * row + rhs]
        held[...] = right_ref[row : row + half, 0, :]
        for k in range(held.shape[1] // rank):
            out[rhs + k * half : rhs + (k + 1) * half] = held[:, k * rank : (k + 1) * rank]


def order_body(pick, *rest):
    pieces, (out, value) = rest[:-2], rest[-2:]
    rhs = out.shape[0]
    half = rhs // 2
    rows = pieces[0].shape[-1]
    whole = [ref for ref in pieces if len(ref.shape) == 3]
    for o, ref in enumerate(whole):
        value[:, o * rows : (o + 1) * rows] = ref[:, 0, :]
    for j, ref in enumerate(pieces[len(whole) :]):
        rank = ref.shape[1]
        for k in range(rows // rank):
            column = len(whole) * rows + k * rank
            value[j * half : (j + 1) * half, column : column + rank] = ref[
                rhs + k * half : rhs + (k + 1) * half
            ]
    both = one_pass(jnp.concatenate(halves(value[...]), axis=0), pick[...], ((1,), (0,)))
    out[...] = both[:rhs] + both[rhs:]


def collect(count, pieces, whole):
    rhs = whole.shape[0] // 2
    part = rhs // count
    for o in range(count):
        row = pl.multiple_of(peer(o) * part, part)
        whole[pl.ds(row, part)] = pieces[o][:part]
        whole[pl.ds(pl.multiple_of(rhs + row, part), part)] = pieces[o][part:]


def weights_body(basis_ref, trans_ref, lift_ref, again_ref, term_ref):
    basis = halves(basis_ref[0, 0])
    trans = halves(trans_ref[0, 0])
    lift = mm(basis, trans)
    lift_ref[...] = lift
    again = mm(halves(lift), basis, ((0,), (0,)))
    again_ref[...] = again
    term_ref[...] = mm(halves(again), trans)


def before_body(last, basis_ref, trans_ref, near_ref, base_ref, right_ref, *outs):
    rhs = right_ref.shape[0]
    new_ref = outs[0]
    basis = halves(basis_ref[0, 0])
    new_ref[...] = base_ref[...] - relax_step * mm_t(halves(near_ref[...]), basis)
    new_ref[:rhs] = new_ref[:rhs] + relax_step * right_ref[...]
    if not last:
        ab = mm(halves(new_ref[...]), basis)
        outs[1][...] = ab
        outs[2][...] = mm(halves(ab), halves(trans_ref[0, 0]))


def terms_body(count, weight_ref, before_ref, *rest):
    pieces, rest = rest[:count], rest[count:]
    outs, (whole, term) = rest[:count], rest[count:]
    collect(count, pieces, whole)
    term[...] = before_ref[...] - relax_step * mm(halves(whole[...]), halves(weight_ref[...]))
    send_quarters(term, count, outs)


def coeffs_body(count, weight_ref, before_ref, *rest):
    pieces, (out, whole) = rest[:count], rest[count:]
    collect(count, pieces, whole)
    out[...] = before_ref[...] - relax_step * mm(halves(whole[...]), halves(weight_ref[...]))


def points_body(count, last, lift_ref, new_ref, *rest):
    pieces, (*outs, whole) = rest[:count], rest[count:]
    collect(count, pieces, whole)
    new = new_ref[...] - relax_step * mm_t(halves(whole[...]), halves(lift_ref[...]))
    if last:
        rhs = new.shape[0] // 2
        outs[0][:, 0, :] = new[:rhs]
        outs[1][:, 0, :] = new[rhs:]
    else:
        outs[0][...] = new


def join_body(*refs):
    for k, ref in enumerate(refs[:-1]):
        refs[-1][k * ref.shape[0] : (k + 1) * ref.shape[0]] = ref[...]


def body(
    right_side,
    tree_order,
    x_start,
    tangent_start,
    dense_kernel,
    dense_deriv,
    leaf_basis,
    transfer,
    sibling_kernel,
    sibling_deriv,
    partner_list,
    parent_kernel,
    parent_deriv,
):
    count = lax.axis_size("sib")
    wide = lax.axis_size("wide")
    rhs = x_start.shape[0]
    leaf = x_start.shape[2]
    rank = leaf_basis.shape[3]
    partners = partner_list.shape[1]
    part = rhs // count
    unit = 2 * rhs * rank * rank

    def sib_from(value, o):
        return lax.ppermute(value, "sib", [(i, i ^ o) for i in range(count)])

    def wide_from(value, k):
        return lax.ppermute(value, "wide", [(i, i ^ k) for i in range(wide)])

    quarter = (2 * part, rank)
    both = (2 * rhs, rank)
    points = (2 * rhs, leaf)
    depth = leaf // rank

    def siblings(values):
        got = {}
        for o in reversed(range(1, count)):
            got[o] = sib_from(values[o], o)
        return [got[o] for o in range(1, count)]

    loaded = (x_start, tangent_start, leaf_basis, transfer)
    leaf_basis, transfer, xs, ab, *terms = call(
        functools.partial(start_kernel, count),
        loaded,
        (leaf_basis.shape, transfer.shape, points, both) + (quarter,) * count,
        unit * (2 * depth + 2),
        scratch=[pltpu.VMEM(both, f32)]
        + [pltpu.VMEM(item.shape, f32) for item in loaded]
        + [pltpu.SemaphoreType.DMA((len(loaded),))],
        specs=[HBM] * len(loaded),
        grant=LARGE,
    )
    packed = count == 4
    if packed:
        near_right = [sib_from(right_side, o) for o in (1, 2)]
        near_ab = [sib_from(ab, o) for o in (1, 2)]
        corners = call(
            pack_body,
            near_right + near_ab,
            ((rhs + rhs * depth // 2, rank),) * 2,
            unit // count,
            scratch=(pltpu.VMEM((rhs // 2, leaf), f32),),
        )
        corners = [sib_from(corners[0], 2), sib_from(corners[1], 1)]
        got_right = [right_side] + near_right + corners
    else:
        got_right = [right_side] + siblings([right_side] * count)
    lift, again_weight, term_weight = call(
        weights_body,
        (leaf_basis, transfer),
        ((leaf, rank), (rank, rank), (rank, rank)),
        unit * 4 * depth,
    )
    (pick,) = call(
        functools.partial(pick_body, count),
        (tree_order,),
        ((count * leaf, leaf),),
        unit * depth,
        kind=bf16,
    )
    right = None
    for step in range(ITERS):
        last = step == ITERS - 1
        got_terms = [terms[0]] + siblings(terms)
        (mine,) = call(sum_kernel, got_terms, (quarter,), unit // count)
        away = {}
        for k in reversed(range(1, wide // 2)):
            away[k] = wide_from(mine, 2 * k)
        away = [away[k] for k in range(1, wide // 2)]
        twin = wide_from(mine, 1)
        if packed and step == 0:
            got_ab, sizes = near_ab + corners, [1, 1, 2]
        else:
            got_ab, sizes = siblings([ab] * count), [1] * (count - 1)
        (joined,) = call(join_body, away, (((wide // 2 - 1) * 2 * part, rank),), unit // count)
        twins = wide_from(joined, 1)
        (base,) = call(
            local_kernel, (xs, dense_kernel, dense_deriv), (points,), unit * 3 * depth * depth
        )
        if right is None:
            (right,) = call(
                order_body,
                [pick] + got_right,
                ((rhs, leaf),),
                unit * depth * depth * count,
                scratch=(pltpu.VMEM((rhs, count * leaf), f32),),
            )
        (near,) = call(
            functools.partial(sibling_body, sizes),
            [sibling_kernel, sibling_deriv] + got_ab,
            (both,),
            unit * 3 * (count - 1),
        )
        before = call(
            functools.partial(before_body, last),
            [leaf_basis, transfer, near, base, right],
            (points,) if last else (points, both, both),
            unit * 4 * depth,
        )
        (field,) = call(
            functools.partial(parent_kernel_body, wide),
            [partner_list, parent_kernel, parent_deriv, mine, joined, twin, twins],
            (quarter,),
            unit * 3 * partners // count,
            scratch=(pltpu.VMEM((wide,) + quarter, f32),),
        )
        got_field = [field] + siblings([field] * count)
        whole = pltpu.VMEM(both, f32)
        if not last:
            terms = call(
                functools.partial(terms_body, count),
                [term_weight, before[2]] + got_field,
                (quarter,) * count,
                unit * 2,
                scratch=(whole, whole),
            )
            (ab,) = call(
                functools.partial(coeffs_body, count),
                [again_weight, before[1]] + got_field,
                (both,),
                unit * 2,
                scratch=(whole,),
            )
        shape = ((rhs, 1, leaf),) * 2 if last else (points,)
        xs, *more = call(
            functools.partial(points_body, count, last),
            [lift, before[0]] + got_field,
            shape,
            unit * 2 * depth,
            scratch=(whole,),
        )
    return xs, more[0]


def solution(mesh):
    placed = (
        P(None, "wide", "sib"),
        P("wide", "sib"),
        P(None, "wide", "sib"),
        P(None, "wide", "sib"),
        P("wide", "sib", None, None),
        P("wide", "sib", None, None),
        P("wide", "sib", None, None),
        P("wide", "sib", None, None),
        P("wide", "sib", None, None, None),
        P("wide", "sib", None, None, None),
        P("wide", None),
        P("wide", None, None, None),
        P("wide", None, None, None),
    )
    return jax.shard_map(
        body,
        mesh=mesh,
        in_specs=placed,
        out_specs=(P(None, "wide", "sib"), P(None, "wide", "sib")),
        check_vma=False,
    )
```
